32 devices in a mesh: code: 4 (over y, core), tok: 8 (over z, x).
Axes of the slice: x: 2, y: 2, z: 4, core: 2. Of those that a mesh axis runs over, the one named last changes fastest.
Arguments:
- tokens: bfloat16 [4096, 256], P('tok'), may hold values from -6 to 6
- codebook: bfloat16 [65536, 256], P('code'), may hold values from -2 to 2
- cotangent: bfloat16 [4096, 256], P('tok'), may hold values from -96 to 96
Outputs:
- quantized: float32 [4096, 256], P('tok', 'code')
- code_grad: float32 [65536, 256], P(('code', 'tok'))
The draws below stay inside these ranges and needn't reach their ends.
All inputs are finite; a program needn't handle non-finite values.
Results may differ from the reference program's by a relative error of at most 0.006.
Values may be sent and summed in bfloat16 or wider, within the bound.
A program may use at most 128 MiB of HBM per device.

```python
import math
import jax
import jax.numpy as jnp
from jax import lax

D = 256
K = 65536
TOKENS = 4096
N_CODE = 4


def base_codebook(key):
    sub = jax.random.fold_in(key, 11)
    unit = jax.random.uniform(sub, (K, D), jnp.float32, -1.0, 1.0)
    return 2.0 * unit


def draw_codebook(key, part):
    return base_codebook(key).astype(jnp.bfloat16)


def draw_tokens(key, part):
    sub = jax.random.fold_in(key, 23)
    values = jnp.clip(jax.random.normal(sub, (TOKENS, D), jnp.float32), -6.0, 6.0)
    return values.astype(jnp.bfloat16)


def block_scale(key, dims, shards, smallest, high):
    gain, own = 1.0, jax.random.fold_in(key, 6)
    for axis_at, blocks in shards:
        draws = jnp.exp(jax.random.uniform(jax.random.fold_in(own, axis_at), (blocks,), jnp.float32, smallest / len(shards), high / len(shards)))
        gain = gain * jnp.repeat(draws, dims[axis_at] // blocks).reshape([-1 if axis == axis_at else 1 for axis in range(len(dims))])
    return gain


def noise(key, dims, scale, bound, split=(), held_as=jnp.bfloat16):
    gain = block_scale(key, dims, split, -0.22, 0.18) if split else 1.0
    entries = jax.random.normal(key, dims, jnp.float32) * scale * gain
    return jnp.minimum(jnp.maximum(entries, -bound), bound).astype(held_as)


def setup_inputs(seed: int = 0) -> dict:
    arg_keys = jax.random.split(jax.random.key(seed), 4)
    tokens = draw_tokens(jax.random.fold_in(arg_keys[3], 71), 0)
    codebook = draw_codebook(jax.random.fold_in(arg_keys[3], 71), 0)
    cotangent = noise(arg_keys[2], (TOKENS, D), 16.0, 96.0, ((0, 8),))
    return dict(tokens=tokens, codebook=codebook, cotangent=cotangent)


def reference(tokens, codebook, cotangent):
    width = tokens.shape[1]
    codes = codebook.shape[0]
    groups = N_CODE
    per_group = codes // groups
    scale = 2.0 / math.sqrt(width)
    block = min(512, tokens.shape[0])
    blocks = tokens.shape[0] // block
    book_wide = codebook.astype(jnp.float32).reshape(groups, per_group, width)

    def forward(index):
        feats = lax.dynamic_slice_in_dim(tokens, index * block, block, 0)
        grads = lax.dynamic_slice_in_dim(cotangent, index * block, block, 0)
        logits = scale * jnp.dot(feats, codebook.T, preferred_element_type=jnp.float32)
        scores = jnp.dot(grads, codebook.T, preferred_element_type=jnp.float32)
        grouped = logits.reshape(block, groups, per_group)
        group_max = lax.optimization_barrier(jnp.max(grouped, axis=2))
        weights = jnp.exp(grouped - group_max[:, :, None]).astype(jnp.bfloat16)
        wide = weights.astype(jnp.float32)
        group_sum = lax.optimization_barrier(jnp.sum(wide, axis=2))
        group_dot = lax.optimization_barrier(jnp.sum(wide * scores.reshape(block, groups, per_group), axis=2))
        group_vec = jnp.einsum('bgk,gkd->bgd', wide, book_wide)
        row_max = lax.optimization_barrier(jnp.max(group_max, axis=1))
        factor = jnp.exp(group_max - row_max[:, None])
        total = lax.optimization_barrier(jnp.sum(factor * group_sum, axis=1))
        inner = lax.optimization_barrier(jnp.sum(factor * group_dot, axis=1)) / total
        quant = lax.optimization_barrier(jnp.sum(factor[:, :, None] * group_vec, axis=1)) / total[:, None]
        return (quant, row_max, total, inner)
    quant, row_max, total, inner = lax.map(forward, jnp.arange(blocks))
    quantized = quant.reshape(tokens.shape[0], width)

    def backward(acc, index):
        feats = lax.dynamic_slice_in_dim(tokens, index * block, block, 0)
        grads = lax.dynamic_slice_in_dim(cotangent, index * block, block, 0)
        logits = scale * jnp.dot(feats, codebook.T, preferred_element_type=jnp.float32)
        scores = jnp.dot(grads, codebook.T, preferred_element_type=jnp.float32)
        prob = jnp.exp(logits - row_max[index][:, None]) / total[index][:, None]
        dlogits = prob * (scores - inner[index][:, None])
        term = jnp.dot(prob.astype(jnp.bfloat16).T, grads, preferred_element_type=jnp.float32)
        term = term + scale * jnp.dot(dlogits.astype(jnp.bfloat16).T, feats, preferred_element_type=jnp.float32)
        return (acc + term, None)
    code_grad, unused = lax.scan(backward, jnp.zeros((codes, width), jnp.float32), jnp.arange(blocks))
    return (quantized, code_grad)
```

```python
import functools
import math

import jax
import jax.numpy as jnp
from jax import lax
from jax.experimental import pallas as pl
from jax.experimental.pallas import tpu as pltpu
from jax.sharding import PartitionSpec as P

LOG2E = 1.4426950408889634
NT = (((1,), (1,)), ((), ()))
RELAY_AFTER = {3: 1, 5: 2, 6: 3, 8: 4}
HANDOVER_AFTER = {5: 1, 7: 2, 8: 3}


def kernel(n_code, n_tok, tile, height, scale, tok_ref, cot_ref, book_hbm, quant_out, grad_out,
           book, slab, peak, total, vec, all_tok, all_cot, stat, final, q_send, q_recv,
           book_sem, own_sem, send1, recv1, send2, recv2, send3, recv3, s_send, s_recv, f_send, f_recv,
           qs_sem, qr_sem):
    mine_code = lax.axis_index("code")
    mine_tok = lax.axis_index("tok")
    rows, width = tok_ref.shape
    codes = book_hbm.shape[0]
    count = codes // tile
    parts = book_sem.shape[0]
    chunk = codes // parts
    per = chunk // tile
    rate = scale * LOG2E
    piece = rows // n_code
    columns = width // n_code

    book_copies = [
        pltpu.make_async_copy(
            book_hbm.at[pl.ds(i * chunk, chunk)], book.at[pl.ds(i * chunk, chunk)], book_sem.at[i]
        )
        for i in range(parts)
    ]
    for c in book_copies:
        c.start()

    barrier = pltpu.get_barrier_semaphore()
    for d in range(1, n_tok):
        pl.semaphore_signal(
            barrier, inc=1, device_id=(mine_code, lax.rem(mine_tok + d, n_tok)),
            device_id_type=pl.DeviceIdType.MESH,
        )
    for c in range(1, n_code):
        pl.semaphore_signal(
            barrier, inc=1, device_id=(lax.rem(mine_code + c, n_code), mine_tok),
            device_id_type=pl.DeviceIdType.MESH,
        )
    pl.semaphore_wait(barrier, n_tok - 1 + n_code - 1)

    def remote(src, dst, send, recv, code, tok):
        return pltpu.make_async_remote_copy(
            src_ref=src, dst_ref=dst, send_sem=send, recv_sem=recv,
            device_id=(code, tok), device_id_type=pl.DeviceIdType.MESH,
        )

    def first_copies(d):
        at = pl.ds(pl.multiple_of(mine_code * piece, piece), piece)
        to = lax.rem(mine_tok + d, n_tok)
        return [
            remote(ref.at[at], every.at[mine_tok, at], send1.at[d - 1, j], recv1.at[d - 1, j], mine_code, to)
            for j, (ref, every) in enumerate(((tok_ref, all_tok), (cot_ref, all_cot)))
        ]

    n_far = n_code // 2
    partner = mine_code + 1 - 2 * lax.rem(mine_code, 2)

    def pass_on(d, k, send, recv, to):
        owner = lax.rem(mine_code - 2 * k + n_code, n_code)
        at = pl.ds(pl.multiple_of(owner * piece, piece), piece)
        block = lax.rem(mine_tok - d + n_tok, n_tok)
        return [
            remote(every.at[block, at], every.at[block, at], send.at[j], recv.at[j], to, mine_tok)
            for j, every in enumerate((all_tok, all_cot))
        ]

    def far_copies(d, k):
        to = lax.rem(mine_code + 2 * k, n_code)
        return pass_on(d, 0, send2.at[d - 1, k - 1], recv2.at[d - 1, k - 1], to)

    def near_copies(d, k):
        return pass_on(d, k, send3.at[d - 1, k], recv3.at[d - 1, k], partner)

    for d in range(1, n_tok):
        for copy in first_copies(d):
            copy.start()
    own = [
        pltpu.make_async_copy(tok_ref, all_tok.at[mine_tok], own_sem.at[0]),
        pltpu.make_async_copy(cot_ref, all_cot.at[mine_tok], own_sem.at[1]),
    ]
    for copy in own:
        copy.start()

    def relay(d):
        for copy in first_copies(d):
            copy.wait_recv()
        for k in range(1, n_far):
            for copy in far_copies(d, k):
                copy.start()
        for copy in near_copies(d, 0):
            copy.start()

    def hand_over(d):
        for k in range(1, n_far):
            for copy in far_copies(d, k):
                copy.wait_recv()
            for copy in near_copies(d, k):
                copy.start()

    def produce(index, slot):
        part_rows = book[pl.ds(pl.multiple_of(index * tile, tile), tile), :]
        logits = lax.dot_general(tok_ref[...], part_rows, NT, preferred_element_type=jnp.float32)
        slab[slot] = logits
        top = logits[:, 0:128]
        for j in range(1, tile // 128):
            top = jnp.maximum(top, logits[:, j * 128:(j + 1) * 128])
        return jnp.broadcast_to(jnp.max(top, axis=1, keepdims=True) * rate, top.shape)

    def consume(index, slot, new):
        old = peak[...]
        fresh = jnp.maximum(old, new)
        peak[...] = fresh
        alpha = jnp.exp2(old - fresh)
        part = total[...] * alpha
        pieces = []
        for j in range(tile // 128):
            w = jnp.exp2(slab[slot, :, j * 128:(j + 1) * 128] * rate - fresh)
            part = part + w
            pieces.append(w.astype(jnp.bfloat16))
        total[...] = part
        weights = jnp.concatenate(pieces, axis=1)
        part_rows = book[pl.ds(pl.multiple_of(index * tile, tile), tile), :]
        update = jnp.dot(weights, part_rows, preferred_element_type=jnp.float32)
        vec[...] = vec[...] * jnp.concatenate([alpha] * (width // 128), axis=1) + update

    peak[...] = jnp.full_like(peak, -1e30)
    total[...] = jnp.zeros_like(total)
    vec[...] = jnp.zeros_like(vec)
    grad_out[...] = jnp.zeros_like(grad_out)
    book_copies[0].wait()
    top = produce(0, 0)
    relayed = handed = 0
    for part in range(parts):
        first = part * per
        last = part + 1 == parts
        if not last:
            book_copies[part + 1].wait()

        def pair(step, top):
            index = first + 2 * step
            nxt = produce(index + 1, 1)
            consume(index, 0, top)
            after = produce(index + 2, 0)
            consume(index + 1, 1, nxt)
            return after

        turns = per // 2 - (1 if last else 0)
        if turns == 1:
            top = pair(0, top)
        elif turns > 1:
            top = lax.fori_loop(0, turns, pair, top)
        if last:
            nxt = produce(count - 1, 1)
            consume(count - 2, 0, top)
            consume(count - 1, 1, nxt)
        d = RELAY_AFTER.get(part + 1)
        if d is not None and d < n_tok:
            relay(d)
            relayed = d
        d = HANDOVER_AFTER.get(part + 1)
        if d is not None and d < n_tok:
            hand_over(d)
            handed = d

    dot = jnp.sum(vec[...] * cot_ref[...].astype(jnp.float32), axis=1, keepdims=True)
    summed = jnp.sum(total[...], axis=1, keepdims=True)
    lane = lax.broadcasted_iota(jnp.int32, (rows, 128), 1)
    packed = jnp.where(lane == 0, peak[...], jnp.where(lane == 1, summed, dot))
    stat[mine_code] = jnp.transpose(packed)[0:8, :]

    def stat_copy(c):
        return remote(stat.at[mine_code], stat.at[mine_code], s_send.at[c - 1], s_recv.at[c - 1],
                      lax.rem(mine_code + c, n_code), mine_tok)

    for c in range(1, n_code):
        stat_copy(c).start()
    for c in range(1, n_code):
        stat_copy(c).wait_recv()
    row_max = stat[0, 0:1, :]
    for c in range(1, n_code):
        row_max = jnp.maximum(row_max, stat[c, 0:1, :])
    norm = jnp.zeros_like(row_max)
    dots = jnp.zeros_like(row_max)
    for c in range(n_code):
        factor = jnp.exp2(stat[c, 0:1, :] - row_max)
        norm = norm + factor * stat[c, 1:2, :]
        dots = dots + factor * stat[c, 2:3, :]
    shift = row_max + jnp.log(norm) * LOG2E
    inner = dots / norm
    row = lax.broadcasted_iota(jnp.int32, (8, rows), 0)
    final[mine_tok] = jnp.where(row == 0, shift, inner)

    def final_copy(d):
        return remote(final.at[mine_tok], final.at[mine_tok], f_send.at[d - 1], f_recv.at[d - 1],
                      mine_code, lax.rem(mine_tok + d, n_tok))

    for d in range(1, n_tok):
        final_copy(d).start()

    gain = jnp.exp2(stat[mine_code, 0:1, :] - shift)
    turned = jnp.transpose(vec[...]) * gain
    for c in range(n_code):
        q_send[c] = turned[c * columns:(c + 1) * columns, :]

    def quant_copy(c):
        to = lax.rem(mine_code + c, n_code)
        return remote(q_send.at[to], q_recv.at[c - 1], qs_sem.at[c - 1], qr_sem.at[c - 1], to, mine_tok)

    for copy in own:
        copy.wait()

    group = grad_out.shape[0]
    base = mine_tok * group

    def block_step(step, carry):
        @pl.when(step + relayed + 1 < n_tok)
        def _():
            relay(step + relayed + 1)

        @pl.when(step + handed + 1 < n_tok)
        def _():
            hand_over(step + handed + 1)

        @pl.when(step == n_tok // 2)
        def _():
            for c in range(1, n_code):
                quant_copy(c).start()

        @pl.when(step > 0)
        def _():
            final_copy(step).wait_recv()
            for k in range(n_far):
                for copy in near_copies(step, k):
                    copy.wait_recv()

        block = lax.rem(mine_tok - step + n_tok, n_tok)
        tok = all_tok[block]
        cot = all_cot[block]
        move = final[block, 0:1, :]
        middle = final[block, 1:2, :]
        other = jnp.concatenate([cot, (tok.astype(jnp.float32) * scale).astype(jnp.bfloat16)], axis=0)

        def half(h, carry):
            at = pl.ds(pl.multiple_of(h * height, height), height)
            codes_at = book[pl.ds(pl.multiple_of(base + h * height, height), height), :]
            logits = lax.dot_general(codes_at, tok, NT, preferred_element_type=jnp.float32)
            scores = lax.dot_general(codes_at, cot, NT, preferred_element_type=jnp.float32)
            prob = jnp.exp2(logits * rate - move)
            dlog = prob * (scores - middle)
            both = jnp.concatenate([prob.astype(jnp.bfloat16), dlog.astype(jnp.bfloat16)], axis=1)
            grad_out[at, :] += jnp.dot(both, other, preferred_element_type=jnp.float32)
            return carry

        return lax.fori_loop(0, group // height, half, carry)

    lax.fori_loop(0, n_tok, block_step, 0)

    result = q_send[mine_code]
    for c in range(1, n_code):
        quant_copy(c).wait_recv()
        result = result + q_recv[c - 1]
    quant_out[...] = result
    for c in range(1, n_code):
        quant_copy(c).wait_send()
        stat_copy(c).wait_send()

    def drain(d, carry):
        for copy in first_copies(d):
            copy.wait_send()
        final_copy(d).wait_send()
        for k in range(n_far):
            for copy in near_copies(d, k):
                copy.wait_send()
            if k:
                for copy in far_copies(d, k):
                    copy.wait_send()
        return carry

    lax.fori_loop(1, n_tok, drain, 0)


def per_device(tokens, codebook, cotangent):
    rows, width = tokens.shape
    codes = codebook.shape[0]
    n_code, n_tok = lax.axis_size("code"), lax.axis_size("tok")
    scale = 2.0 / math.sqrt(width)
    group = codes // n_tok
    tile = min(1024, codes // 2)
    parts = min(8, codes // (2 * tile))
    columns = width // n_code
    dma = pltpu.SemaphoreType.DMA
    vmem = pl.BlockSpec(memory_space=pltpu.VMEM)
    turned, grad = pl.pallas_call(
        functools.partial(kernel, n_code, n_tok, tile, min(1024, group), scale),
        out_shape=(
            jax.ShapeDtypeStruct((columns, rows), jnp.float32),
            jax.ShapeDtypeStruct((group, width), jnp.float32),
        ),
        in_specs=[vmem, vmem, pl.BlockSpec(memory_space=pl.ANY)],
        out_specs=(vmem, vmem),
        scratch_shapes=[
            pltpu.VMEM((codes, width), jnp.bfloat16),
            pltpu.VMEM((2, rows, tile), jnp.float32),
            pltpu.VMEM((rows, 128), jnp.float32),
            pltpu.VMEM((rows, 128), jnp.float32),
            pltpu.VMEM((rows, width), jnp.float32),
            pltpu.VMEM((n_tok, rows, width), jnp.bfloat16),
            pltpu.VMEM((n_tok, rows, width), jnp.bfloat16),
            pltpu.VMEM((n_code, 8, rows), jnp.float32),
            pltpu.VMEM((n_tok, 8, rows), jnp.float32),
            pltpu.VMEM((n_code, columns, rows), jnp.float32),
            pltpu.VMEM((n_code - 1, columns, rows), jnp.float32),
            dma((parts,)),
            dma((2,)),
            dma((n_tok - 1, 2)),
            dma((n_tok - 1, 2)),
            dma((n_tok - 1, n_code // 2 - 1, 2)),
            dma((n_tok - 1, n_code // 2 - 1, 2)),
            dma((n_tok - 1, n_code // 2, 2)),
            dma((n_tok - 1, n_code // 2, 2)),
            dma((n_code - 1,)),
            dma((n_code - 1,)),
            dma((n_tok - 1,)),
            dma((n_tok - 1,)),
            dma((n_code - 1,)),
            dma((n_code - 1,)),
        ],
        compiler_params=pltpu.CompilerParams(
            collective_id=0, has_side_effects=True, vmem_limit_bytes=60 * 1024 * 1024
        ),
        cost_estimate=pl.CostEstimate(
            flops=12 * rows * codes * width, bytes_accessed=codes * width * 2,
            transcendentals=2 * rows * codes,
        ),
        name="quantize",
    )(tokens, cotangent, codebook)
    return turned.T, grad


def solution(mesh):
    return jax.shard_map(
        per_device,
        mesh=mesh,
        in_specs=(P("tok", None), P("code", None), P("tok", None)),
        out_specs=(P("tok", "code"), P(("code", "tok"), None)),
        check_vma=False,
    )
```
